16 devices in a mesh: dp: 2 (over y, z), ep: 8 (over x, core).
Axes of the slice: x: 4, y: 2, z: 1, core: 2. Of those that a mesh axis runs over, the one named last changes fastest.
The devices are a block of a 4x4x8 slice.
Arguments:
- x_in: bfloat16 [256, 512, 768], P(('dp', 'ep')), parts along dimension 0
- pad_mask: int32 [256, 512], P(('dp', 'ep')), parts along dimension 0
- rel_bias: float32 [12, 512, 512], replicated
- expert_idx: int32 [2, 256, 512], P(None, ('dp', 'ep')), parts along dimension 1
- norm_scale: float32 [2, 2, 768], replicated
- w_query: bfloat16 [2, 768, 768], replicated
- w_key: bfloat16 [2, 768, 768], replicated
- w_value: bfloat16 [2, 768, 768], replicated
- w_attn_out: bfloat16 [2, 768, 768], replicated
- w_router: float32 [2, 768, 16], replicated
- w_in: bfloat16 [2, 16, 768, 3072], P(None, 'ep')
- w_out: bfloat16 [2, 16, 3072, 768], P(None, 'ep')
Outputs:
- output: bfloat16 [256, 512, 768], P(('dp', 'ep')), parts along dimension 0
There are 2 independent parts. The reference program is written for one: setup_inputs(seed, part) draws one part's arguments, and reference() takes and returns one part's arrays. A program takes and returns all parts, laid end to end along the dimension named above; an argument that names none is the same for every part.
All inputs are finite; a program needn't handle non-finite values.
Results may differ from the reference program's by a relative error of at most 0.0189939.
Values are sent between devices in bfloat16 or wider.
A program may use at most 768 MiB of HBM per device.

```python
import jax
import jax.numpy as jnp
from jax import lax

SEQS = 16
SEQ = 512
D = 768
HEADS = 12
HEAD = 64
FF = 3072
EXPERTS = 16
GROUPS = 8
CAP_FACTOR = 2
NORM_EPS = 1e-6
NEG_BIG = -1e9
TOKENS = SEQS * SEQ
NUM_SEQ = GROUPS * SEQS
INNER = HEADS * HEAD
CAPACITY = (CAP_FACTOR * TOKENS + EXPERTS - 1) // EXPERTS


def draw_mask(rng_key, num_seq):
    lengths = jax.random.randint(rng_key, (num_seq,), SEQ // 4, SEQ + 1)
    return (jnp.arange(SEQ)[None, :] < lengths[:, None]).astype(jnp.int32)


def draw_routes(rng_key, num_seq):
    route_keys = jax.random.split(rng_key, 5)
    rank_draws = [jax.random.randint(route_keys[draw_id], (2, num_seq, SEQ), 0, EXPERTS) for draw_id in range(3)]
    ranks = jnp.minimum(jnp.minimum(rank_draws[0], rank_draws[1]), rank_draws[2])
    perm_first = jax.random.permutation(route_keys[3], EXPERTS)
    perm_second = jax.random.permutation(route_keys[4], EXPERTS)
    return jnp.stack([perm_first[ranks[0]], perm_second[ranks[1]]]).astype(jnp.int32)


def setup_inputs(seed: int = 0, part: int = 0) -> dict:
    base_key = jax.random.key(seed)
    part_keys = jax.random.split(jax.random.fold_in(base_key, part), 3)
    shared_keys = jax.random.split(base_key, 10)
    x_in = jax.random.normal(part_keys[0], (NUM_SEQ, SEQ, D), jnp.float32).astype(jnp.bfloat16)
    pad_mask = draw_mask(part_keys[1], NUM_SEQ)
    expert_idx = draw_routes(part_keys[2], NUM_SEQ)
    rel_bias = 2.0 * jax.random.normal(shared_keys[0], (HEADS, SEQ, SEQ), jnp.float32)
    norm_scale = jax.random.uniform(shared_keys[1], (2, 2, D), jnp.float32, 0.5, 1.5)
    qk_std = (2.0 / D) ** 0.5 * HEAD ** -0.25
    w_query = (qk_std * jax.random.normal(shared_keys[2], (2, D, INNER), jnp.float32)).astype(jnp.bfloat16)
    w_key = (qk_std * jax.random.normal(shared_keys[3], (2, D, INNER), jnp.float32)).astype(jnp.bfloat16)
    w_value = (D ** -0.5 * jax.random.normal(shared_keys[4], (2, D, INNER), jnp.float32)).astype(jnp.bfloat16)
    w_attn_out = (INNER ** -0.5 * jax.random.normal(shared_keys[5], (2, INNER, D), jnp.float32)).astype(jnp.bfloat16)
    w_router = D ** -0.5 * jax.random.normal(shared_keys[6], (2, D, EXPERTS), jnp.float32)
    w_in = (D ** -0.5 * jax.random.normal(shared_keys[7], (2, EXPERTS, D, FF), jnp.float32)).astype(jnp.bfloat16)
    w_out = (EXPERTS * FF ** -0.5 * jax.random.normal(shared_keys[8], (2, EXPERTS, FF, D), jnp.float32)).astype(jnp.bfloat16)
    return dict(x_in=x_in, pad_mask=pad_mask, rel_bias=rel_bias, expert_idx=expert_idx, norm_scale=norm_scale, w_query=w_query, w_key=w_key, w_value=w_value, w_attn_out=w_attn_out, w_router=w_router, w_in=w_in, w_out=w_out)


def rms_norm(hidden, gain):
    hid32 = hidden.astype(jnp.float32)
    return hid32 * lax.rsqrt(jnp.mean(hid32 * hid32, axis=-1, keepdims=True) + NORM_EPS) * gain


def attention_block(hidden, pad_mask, rel_bias, gain, query_w, key_w, value_w, out_w):
    def one_sequence(seq_pair):
        seq_rows, seq_mask = seq_pair
        normed = rms_norm(seq_rows, gain).astype(jnp.bfloat16)
        query_rows = jnp.dot(normed, query_w, preferred_element_type=jnp.float32).astype(jnp.bfloat16).reshape(SEQ, HEADS, HEAD)
        key_rows = jnp.dot(normed, key_w, preferred_element_type=jnp.float32).astype(jnp.bfloat16).reshape(SEQ, HEADS, HEAD)
        value_rows = jnp.dot(normed, value_w, preferred_element_type=jnp.float32).astype(jnp.bfloat16).reshape(SEQ, HEADS, HEAD)
        scores = jnp.einsum('qhd,khd->hqk', query_rows.astype(jnp.float32), key_rows.astype(jnp.float32))
        scores = scores + rel_bias + jnp.where(seq_mask > 0, 0.0, NEG_BIG)[None, None, :]
        attn_probs = jax.nn.softmax(scores, axis=-1).astype(jnp.bfloat16)
        context = jnp.einsum('hqk,khd->qhd', attn_probs.astype(jnp.float32), value_rows.astype(jnp.float32))
        context = context.astype(jnp.bfloat16).reshape(SEQ, INNER)
        attn_out = jnp.dot(context, out_w, preferred_element_type=jnp.float32)
        return (seq_rows.astype(jnp.float32) + attn_out).astype(jnp.bfloat16)
    return lax.map(one_sequence, (hidden, pad_mask))


def expert_block(hidden, layer_ids, gain, route_w, up_w, down_w):
    grouped = hidden.reshape(GROUPS, TOKENS, D)
    ids_grouped = layer_ids.reshape(GROUPS, TOKENS)

    def route_group(grp_pair):
        grp_rows, grp_ids = grp_pair
        normed32 = rms_norm(grp_rows, gain)
        logits = jnp.dot(normed32, route_w, preferred_element_type=jnp.float32)
        gate_val = jnp.take_along_axis(jax.nn.softmax(logits, axis=-1), grp_ids[:, None], axis=1)[:, 0]
        one_hot = (grp_ids[:, None] == jnp.arange(EXPERTS)[None, :]).astype(jnp.int32)
        token_slot = jnp.take_along_axis(jnp.cumsum(one_hot, axis=0), grp_ids[:, None], axis=1)[:, 0] - 1
        flat_slot = jnp.where(token_slot < CAPACITY, grp_ids * CAPACITY + token_slot, EXPERTS * CAPACITY)
        slot_token = jnp.full((EXPERTS * CAPACITY,), TOKENS, jnp.int32).at[flat_slot].set(jnp.arange(TOKENS, dtype=jnp.int32), mode='drop')
        packed = jnp.take(normed32.astype(jnp.bfloat16), slot_token, axis=0, mode='fill', fill_value=0)
        return packed.reshape(EXPERTS, CAPACITY, D), gate_val, flat_slot

    packed, gate_val, flat_slot = lax.map(route_group, (grouped, ids_grouped))

    def one_expert(expert_parts):
        exp_rows, exp_up, exp_down = expert_parts
        flat_rows = exp_rows.reshape(GROUPS * CAPACITY, D)
        inner_act = jnp.maximum(jnp.dot(flat_rows, exp_up, preferred_element_type=jnp.float32), 0.0).astype(jnp.bfloat16)
        return jnp.dot(inner_act, exp_down, preferred_element_type=jnp.float32).astype(jnp.bfloat16).reshape(GROUPS, CAPACITY, D)

    expert_rows = lax.map(one_expert, (jnp.swapaxes(packed, 0, 1), up_w, down_w))
    expert_rows = jnp.swapaxes(expert_rows, 0, 1).reshape(GROUPS, EXPERTS * CAPACITY, D)

    def combine(grp_parts):
        grp_rows, grp_out, grp_gate, grp_flat = grp_parts
        returned = jnp.take(grp_out, grp_flat, axis=0, mode='fill', fill_value=0)
        return (grp_rows.astype(jnp.float32) + grp_gate[:, None] * returned.astype(jnp.float32)).astype(jnp.bfloat16)

    return lax.map(combine, (grouped, expert_rows, gate_val, flat_slot)).reshape(NUM_SEQ, SEQ, D)


def reference(x_in, pad_mask, rel_bias, expert_idx, norm_scale, w_query, w_key, w_value, w_attn_out, w_router, w_in, w_out):
    def layer_step(hidden, layer_params):
        gains, query_w, key_w, value_w, out_w, route_w, up_w, down_w, layer_ids = layer_params
        hidden = attention_block(hidden, pad_mask, rel_bias, gains[0], query_w, key_w, value_w, out_w)
        hidden = expert_block(hidden, layer_ids, gains[1], route_w, up_w, down_w)
        return hidden, None
    final_state = lax.scan(layer_step, x_in, (norm_scale, w_query, w_key, w_value, w_attn_out, w_router, w_in, w_out, expert_idx))
    return final_state[0]
```

```python
import functools

import jax
import jax.numpy as jnp
import numpy as np
from jax import lax
from jax.experimental import pallas as pl
from jax.experimental.pallas import tpu as pltpu
from jax.sharding import PartitionSpec as P

NORM_EPS = 1e-6
NEG_BIG = -1e9
CAP_FACTOR = 2
TILE = 16
BF16 = jnp.bfloat16
F32 = jnp.float32


def neg_pieces():
    pieces, rest = [], np.float32(NEG_BIG)
    for _ in range(3):
        piece = np.float32(np.asarray(rest, jnp.bfloat16))
        pieces.append(float(piece))
        rest = np.float32(rest - piece)
    return pieces


def dot(a, b):
    return jnp.dot(a, b, preferred_element_type=F32)


def dot_t(a, b):
    return lax.dot_general(a, b, (((1,), (1,)), ((), ())), preferred_element_type=F32)


def attention_kernel(x_ref, mask_ref, bias_ref, g0_ref, g1_ref, wq_ref, wk_ref, wv_ref, wo_ref, wr_ref, eid_ref,
                     h1_ref, b_ref, gate_ref, q_s, k_s, v_s, c_s):
    seq, dim = x_ref.shape
    heads = bias_ref.shape[0]
    head = dim // heads
    lanes = 2 * head
    hid = x_ref[...].astype(F32)
    inv = lax.rsqrt(jnp.mean(hid * hid, axis=-1, keepdims=True) + NORM_EPS)
    normed = (hid * inv * g0_ref[...]).astype(BF16)
    q_s[...] = dot(normed, wq_ref[...]).astype(BF16)
    k_s[...] = dot(normed, wk_ref[...]).astype(BF16)
    v_s[...] = dot(normed, wv_ref[...]).astype(BF16)
    lane = lax.broadcasted_iota(jnp.int32, (seq, lanes), 1)
    hi, mid, lo = neg_pieces()
    piece = jnp.where(lane == 0, hi, jnp.where(lane == 1, mid, jnp.where(lane == 2, lo, 0.0)))
    key_mask = jnp.where(mask_ref[...] > 0, 0.0, piece).astype(BF16)
    ones = jnp.ones((seq, lanes), BF16)
    zero = jnp.zeros((seq, lanes), BF16)
    low = lane < head
    for pair in range(heads // 2):
        cols = slice(pair * lanes, (pair + 1) * lanes)
        keys = jnp.concatenate([k_s[:, cols], key_mask], axis=1)
        vals = v_s[:, cols]
        outs = []
        for half in range(2):
            keep = low if half == 0 else jnp.logical_not(low)
            query = jnp.concatenate([jnp.where(keep, q_s[:, cols], zero), ones], axis=1)
            scores = dot_t(query, keys) + bias_ref[2 * pair + half]
            top = jnp.max(scores, axis=-1, keepdims=True)
            probs = jnp.exp(scores - top)
            total = jnp.sum(probs, axis=-1, keepdims=True)
            outs.append(dot(probs.astype(BF16), vals) * (1.0 / total))
        c_s[:, cols] = jnp.where(low, outs[0], outs[1]).astype(BF16)
    h1 = (hid + dot(c_s[...], wo_ref[...])).astype(BF16)
    h1_ref[...] = h1
    hid1 = h1.astype(F32)
    inv1 = lax.rsqrt(jnp.mean(hid1 * hid1, axis=-1, keepdims=True) + NORM_EPS)
    rows = hid1 * inv1 * g1_ref[...]
    rows1 = rows.astype(BF16)
    b_ref[...] = rows1
    rest = rows - rows1.astype(F32)
    rows2 = rest.astype(BF16)
    rows3 = (rest - rows2.astype(F32)).astype(BF16)
    acc = dot(rows1, wr_ref[0]) + (dot(rows2, wr_ref[1]) + dot(rows3, wr_ref[2]))
    nexp = wr_ref.shape[2] // 8
    logits = acc[:, :nexp] + (acc[:, nexp:2 * nexp] + acc[:, 2 * nexp:3 * nexp])
    expo = jnp.exp(logits - jnp.max(logits, axis=-1, keepdims=True))
    ids = lax.broadcasted_iota(jnp.int32, expo.shape, 1)
    picked = jnp.sum(jnp.where(ids == eid_ref[...], expo, 0.0), axis=-1, keepdims=True)
    gate_ref[...] = picked / jnp.sum(expo, axis=-1, keepdims=True)


def attention(hidden, mask_col, rel_bias, g0, g1, wq, wk, wv, wo, wr, eid_col, seq):
    toks, dim = hidden.shape
    heads = rel_bias.shape[0]
    tok_spec = pl.BlockSpec((seq, dim), lambda s: (s, 0))
    col_spec = pl.BlockSpec((seq, 1), lambda s: (s, 0))

    def whole(arr):
        return pl.BlockSpec(arr.shape, lambda s: (0,) * arr.ndim, pipeline_mode=pl.Buffered(1))

    nseq = toks // seq
    return pl.pallas_call(
        attention_kernel,
        grid=(nseq,),
        in_specs=[tok_spec, col_spec, whole(rel_bias), whole(g0), whole(g1), whole(wq), whole(wk), whole(wv), whole(wo),
                  whole(wr), col_spec],
        out_specs=[tok_spec, tok_spec, col_spec],
        out_shape=[jax.ShapeDtypeStruct((toks, dim), BF16), jax.ShapeDtypeStruct((toks, dim), BF16),
                   jax.ShapeDtypeStruct((toks, 1), F32)],
        scratch_shapes=[pltpu.VMEM((seq, dim), BF16)] * 4,
        compiler_params=pltpu.CompilerParams(dimension_semantics=("arbitrary",), vmem_limit_bytes=60 * 2**20),
        cost_estimate=pl.CostEstimate(flops=toks * dim * dim * 8 + toks * seq * dim * 4, bytes_accessed=toks * dim * 6,
                                      transcendentals=toks * seq * heads),
        name="attention",
    )(hidden, mask_col, rel_bias, g0, g1, wq, wk, wv, wo, wr, eid_col)


def pack_kernel(reg_ref, dst_ref, cnt_ref, b_ref, pos_ref, out_ref, acc_s, srt_s, sem, *, nexp, cap):
    step = pl.program_id(0)
    seq, dim = b_ref.shape
    rows = srt_s.shape[0]
    chunk = 256

    @pl.when(step == 0)
    def _():
        def clear(i, carry):
            acc_s[pl.ds(pl.multiple_of(i * chunk, chunk), chunk), :] = jnp.zeros((chunk, dim), BF16)
            return carry
        lax.fori_loop(0, acc_s.shape[0] // chunk, clear, 0)

    pos = pos_ref[0]
    last = step * nexp + nexp - 1
    used = (reg_ref[last] + cnt_ref[last]) * TILE
    for c in range(rows // chunk):
        @pl.when(used > c * chunk)
        def _():
            ids = lax.broadcasted_iota(jnp.int32, (chunk, seq), 0) + c * chunk
            pick = jnp.where(ids == pos, 1.0, 0.0).astype(BF16)
            srt_s[c * chunk:(c + 1) * chunk, :] = dot(pick, b_ref[...]).astype(BF16)

    for e in range(nexp):
        base = step * nexp + e
        src0, dst0 = reg_ref[base] * TILE, dst_ref[base] * TILE + e * cap

        def move(i, carry):
            src = pl.ds(pl.multiple_of(src0 + i * TILE, TILE), TILE)
            dst = pl.ds(pl.multiple_of(dst0 + i * TILE, TILE), TILE)
            acc_s[dst, :] = acc_s[dst, :] + srt_s[src, :]
            return carry
        lax.fori_loop(0, cnt_ref[base], move, 0)

    @pl.when(step == pl.num_programs(0) - 1)
    def _():
        copy = pltpu.make_async_copy(acc_s, out_ref, sem)
        copy.start()
        copy.wait()


def pack(reg, dst, cnt, b, pos_row, nexp, cap):
    toks, dim = b.shape
    nseq, _, seq = pos_row.shape
    rows = seq + 2 * nexp * TILE
    return pl.pallas_call(
        functools.partial(pack_kernel, nexp=nexp, cap=cap),
        grid_spec=pltpu.PrefetchScalarGridSpec(
            num_scalar_prefetch=3,
            grid=(nseq,),
            in_specs=[pl.BlockSpec((seq, dim), lambda s, *_: (s, 0)), pl.BlockSpec((1, 1, seq), lambda s, *_: (s, 0, 0))],
            out_specs=pl.BlockSpec(memory_space=pl.ANY),
            scratch_shapes=[pltpu.VMEM((nexp * cap, dim), BF16), pltpu.VMEM((rows, dim), BF16), pltpu.SemaphoreType.DMA(())],
        ),
        out_shape=jax.ShapeDtypeStruct((nexp * cap, dim), BF16),
        compiler_params=pltpu.CompilerParams(dimension_semantics=("arbitrary",), vmem_limit_bytes=60 * 2**20),
        cost_estimate=pl.CostEstimate(flops=2 * nseq * rows * seq * dim, bytes_accessed=nexp * cap * dim * 2, transcendentals=0),
        name="pack",
    )(reg, dst, cnt, b, pos_row)


def combine_kernel(reg_ref, dst_ref, cnt_ref, ret_ref, h1_ref, gate_ref, pos_ref, out_ref, srt_s, *, nexp, cap):
    step = pl.program_id(0)
    seq, dim = h1_ref.shape
    rows = srt_s.shape[0]

    @pl.when(step == 0)
    def _():
        srt_s[...] = jnp.zeros_like(srt_s)

    for e in range(nexp):
        base = step * nexp + e
        src0, dst0 = reg_ref[base] * TILE, dst_ref[base] * TILE + e * cap

        def move(i, carry):
            src = pl.ds(pl.multiple_of(src0 + i * TILE, TILE), TILE)
            dst = pl.ds(pl.multiple_of(dst0 + i * TILE, TILE), TILE)
            srt_s[src, :] = ret_ref[dst, :]
            return carry
        lax.fori_loop(0, cnt_ref[base], move, 0)

    ids = lax.broadcasted_iota(jnp.int32, (seq, rows), 1)
    pick = jnp.where(ids == pos_ref[...], 1.0, 0.0).astype(BF16)
    back = dot(pick, srt_s[...])
    out_ref[...] = (h1_ref[...].astype(F32) + gate_ref[...] * back).astype(BF16)


def combine(reg, dst, cnt, returned, h1, gate, pos_col, nexp, cap, seq):
    toks, dim = h1.shape
    rows = seq + 2 * nexp * TILE
    tok_spec = pl.BlockSpec((seq, dim), lambda s, *_: (s, 0))
    col_spec = pl.BlockSpec((seq, 1), lambda s, *_: (s, 0))
    return pl.pallas_call(
        functools.partial(combine_kernel, nexp=nexp, cap=cap),
        grid_spec=pltpu.PrefetchScalarGridSpec(
            num_scalar_prefetch=3,
            grid=(toks // seq,),
            in_specs=[pl.BlockSpec(returned.shape, lambda s, *_: (0, 0), pipeline_mode=pl.Buffered(1)), tok_spec, col_spec, col_spec],
            out_specs=tok_spec,
            scratch_shapes=[pltpu.VMEM((rows, dim), BF16)],
        ),
        out_shape=jax.ShapeDtypeStruct((toks, dim), BF16),
        compiler_params=pltpu.CompilerParams(dimension_semantics=("arbitrary",), vmem_limit_bytes=60 * 2**20),
        cost_estimate=pl.CostEstimate(flops=2 * toks * rows * dim, bytes_accessed=nexp * cap * dim * 2, transcendentals=0),
        name="combine",
    )(reg, dst, cnt, returned, h1, gate, pos_col)


def peer_of(k, count):
    me = lax.axis_index('ep')
    chip, core = me // 2, me % 2
    return ((chip + k // 2) % (count // 2)) * 2 + (core + k % 2) % 2


def source_of(k, count):
    me = lax.axis_index('ep')
    chip, core = me // 2, me % 2
    return ((chip + count // 2 - k // 2) % (count // 2)) * 2 + (core + k % 2) % 2


def exchange_kernel(packed_ref, up_ref, down_ref, ret_ref, recv_s, up_s, down_s, acc_s, w_sem, send_sem, recv_sem, back_sem, home_sem,
                    *, layer, count, local, block):
    cap, dim = packed_ref.shape[1], packed_ref.shape[2]
    inner = up_s.shape[2]
    halves = cap // block
    pieces = local * halves
    step = min(inner, 768)
    me = lax.axis_index('ep')

    def part(p):
        return p // halves, pl.ds(pl.multiple_of((p % halves) * block, block), block)

    def outgoing(k, p):
        peer = peer_of(k, count)
        j, rows = part(p)
        return pltpu.make_async_remote_copy(
            src_ref=packed_ref.at[peer * local + j, rows], dst_ref=recv_s.at[k, j, rows], send_sem=send_sem.at[k, p],
            recv_sem=recv_sem.at[k, p], device_id={'ep': peer}, device_id_type=pl.DeviceIdType.MESH)

    def homing(k, p):
        j, rows = part(p)
        return pltpu.make_async_remote_copy(
            src_ref=recv_s.at[k, j, rows], dst_ref=ret_ref.at[me * local + j, rows], send_sem=back_sem.at[k, p],
            recv_sem=home_sem.at[k, p], device_id={'ep': source_of(k, count)}, device_id_type=pl.DeviceIdType.MESH)

    def own_in(p):
        j, rows = part(p)
        return pltpu.make_async_copy(packed_ref.at[me * local + j, rows], recv_s.at[0, j, rows], recv_sem.at[0, p])

    def own_out(p):
        j, rows = part(p)
        return pltpu.make_async_copy(recv_s.at[0, j, rows], ret_ref.at[me * local + j, rows], back_sem.at[0, p])

    def weights(j):
        return (pltpu.make_async_copy(up_ref.at[layer, j], up_s.at[j], w_sem.at[0, j]),
                pltpu.make_async_copy(down_ref.at[layer, j], down_s.at[j], w_sem.at[1, j]))

    barrier = pltpu.get_barrier_semaphore()
    for k in range(1, count):
        pl.semaphore_signal(barrier, inc=1, device_id={'ep': peer_of(k, count)}, device_id_type=pl.DeviceIdType.MESH)
    pl.semaphore_wait(barrier, count - 1)

    def start_out(i, carry):
        outgoing(1 + i % (count - 1), i // (count - 1)).start()
        return carry
    lax.fori_loop(0, pieces * (count - 1), start_out, 0)
    for p in range(pieces):
        own_in(p).start()
    for j in range(local):
        for copy in weights(j):
            copy.start()
    for j in range(local):
        for copy in weights(j):
            copy.wait()

    def order(t):
        u = jnp.maximum(t - pieces, 0)
        own = t < pieces
        return jnp.where(own, 0, 1 + u % (count - 1)), jnp.where(own, t, u // (count - 1))

    def send_back(t):
        @pl.when(t < pieces)
        def _():
            own_out(t).start()

        @pl.when(t >= pieces)
        def _():
            u = t - pieces
            homing(1 + u % (count - 1), u // (count - 1)).start()

    def work(t, carry):
        @pl.when(t < pieces)
        def _():
            own_in(t).wait()

        @pl.when(t >= pieces)
        def _():
            u = t - pieces
            outgoing(1 + u % (count - 1), u // (count - 1)).wait_recv()

        k, p = order(t)
        j, rows = part(p)
        x = recv_s[k, j, rows, :]
        for f in range(0, inner, step):
            act = jnp.maximum(dot(x, up_s[j, :, f:f + step]), 0.0).astype(BF16)
            piece = dot(act, down_s[j, f:f + step, :])
            acc_s[...] = piece if f == 0 else acc_s[...] + piece
        recv_s[k, j, rows, :] = acc_s[...].astype(BF16)

        @pl.when(t > 0)
        def _():
            send_back(t - 1)
        return carry
    total = pieces * count
    lax.fori_loop(0, total, work, 0)
    send_back(total - 1)

    def drain(i, carry):
        k, p = 1 + i % (count - 1), i // (count - 1)
        outgoing(k, p).wait_send()
        back = homing(k, p)
        back.wait_send()
        back.wait_recv()
        return carry
    lax.fori_loop(0, pieces * (count - 1), drain, 0)
    for p in range(pieces):
        own_out(p).wait()


def exchange_ffn(packed, w_in, w_out, layer, count, block=512):
    nexp, cap, dim = packed.shape
    local, inner = w_in.shape[1], w_in.shape[3]
    pieces = local * (cap // block)
    dma = pltpu.SemaphoreType.DMA
    return pl.pallas_call(
        functools.partial(exchange_kernel, layer=layer, count=count, local=local, block=block),
        in_specs=[pl.BlockSpec(memory_space=pl.ANY)] * 3,
        out_specs=pl.BlockSpec(memory_space=pl.ANY),
        out_shape=jax.ShapeDtypeStruct(packed.shape, BF16),
        scratch_shapes=[pltpu.VMEM((count, local, cap, dim), BF16), pltpu.VMEM((local, dim, inner), BF16),
                        pltpu.VMEM((local, inner, dim), BF16), pltpu.VMEM((block, dim), F32), dma((2, local)),
                        dma((count, pieces)), dma((count, pieces)), dma((count, pieces)), dma((count, pieces))],
        compiler_params=pltpu.CompilerParams(collective_id=layer, has_side_effects=True, vmem_limit_bytes=60 * 2**20),
        cost_estimate=pl.CostEstimate(flops=4 * nexp * cap * dim * inner, bytes_accessed=nexp * cap * dim * 4, transcendentals=0),
        name="exchange_ffn",
    )(packed, w_in, w_out)


def routing(expert_idx, nexp, cap):
    layers, nseq, seq = expert_idx.shape
    hot = expert_idx[..., None] == jnp.arange(nexp, dtype=jnp.int32)
    tri = (jnp.arange(seq)[:, None] > jnp.arange(seq)[None, :]).astype(BF16)
    before = jnp.einsum('ut,lste->lsue', tri, hot.astype(BF16), preferred_element_type=F32).astype(jnp.int32)
    count = jnp.sum(hot.astype(jnp.int32), axis=2)
    prior = jnp.arange(nseq)[:, None] > jnp.arange(nseq)[None, :]
    start = jnp.sum(jnp.where(prior[None, :, :, None], count[:, None], 0), axis=2)
    kept = jnp.clip(cap - start, 0, count)
    off = start % TILE
    tiles = jnp.where(kept > 0, (off + kept + TILE - 1) // TILE, 0)
    lower = jnp.arange(nexp)[:, None] > jnp.arange(nexp)[None, :]
    reg = jnp.sum(jnp.where(lower[None, None], tiles[:, :, None, :], 0), axis=3)
    dst = jnp.minimum(start, cap - 1) // TILE
    place = jnp.where(before < kept[:, :, None, :], (reg * TILE + off)[:, :, None, :] + before, 1 << 20)
    pos = jnp.sum(jnp.where(hot, place, 0), axis=3)
    return reg, dst, tiles, pos


def split_router(w_router):
    layers, dim, nexp = w_router.shape
    w1 = lax.reduce_precision(w_router, 8, 7)
    w2 = lax.reduce_precision(w_router - w1, 8, 7)
    w3 = lax.reduce_precision(w_router - w1 - w2, 8, 7)
    zero = jnp.zeros_like(w1)
    rows = [[w1, w2, w3], [w1, w2, zero], [w1, zero, zero]]
    out = jnp.stack([jnp.concatenate(r + [zero] * 5, axis=2) for r in rows], axis=1)
    return out.astype(BF16)


def solution(mesh):
    token_spec = P(('dp', 'ep'))

    def per_device(x_in, pad_mask, rel_bias, expert_idx, norm_scale, w_query, w_key, w_value, w_attn_out, w_router, w_in, w_out):
        num_seqs, seq_len, model_dim = x_in.shape
        toks = num_seqs * seq_len
        nexp = w_router.shape[2]
        layers = w_router.shape[0]
        cap = (CAP_FACTOR * toks + nexp - 1) // nexp
        local = w_in.shape[1]
        count = nexp // local
        reg, dst, tiles, pos = routing(expert_idx, nexp, cap)
        wr = split_router(w_router)
        mask_col = pad_mask.reshape(toks, 1)
        hidden = x_in.reshape(toks, model_dim)
        for layer in range(layers):
            tables = [t[layer].reshape(num_seqs * nexp) for t in (reg, dst, tiles)]
            h1, b, gate = attention(hidden, mask_col, rel_bias, norm_scale[layer, 0][None], norm_scale[layer, 1][None],
                                    w_query[layer], w_key[layer], w_value[layer], w_attn_out[layer], wr[layer],
                                    expert_idx[layer].reshape(toks, 1), seq_len)
            packed = pack(*tables, b, pos[layer].reshape(num_seqs, 1, seq_len), nexp, cap)
            returned = exchange_ffn(packed.reshape(nexp, cap, model_dim), w_in, w_out, layer, count)
            hidden = combine(*tables, returned.reshape(nexp * cap, model_dim), h1, gate, pos[layer].reshape(toks, 1), nexp, cap, seq_len)
        return hidden.reshape(num_seqs, seq_len, model_dim)

    return jax.shard_map(per_device, mesh=mesh, in_specs=(token_spec, token_spec, P(), P(None, ('dp', 'ep')), P(), P(), P(), P(), P(), P(), P(None, 'ep'), P(None, 'ep')), out_specs=token_spec, check_vma=False)
```

```python
import functools

import jax
import jax.numpy as jnp
import numpy as np
from jax import lax
from jax.experimental import pallas as pl
from jax.experimental.pallas import tpu as pltpu
from jax.sharding import PartitionSpec as P

NORM_EPS = 1e-6
NEG_BIG = -1e9
CAP_FACTOR = 2
TILE = 16
PAIRS_PER_STEP = 1
SHARED = (1, 1)
BF16 = jnp.bfloat16
F32 = jnp.float32


def neg_pieces():
    pieces, rest = [], np.float32(NEG_BIG)
    for _ in range(3):
        piece = np.float32(np.asarray(rest, jnp.bfloat16))
        pieces.append(float(piece))
        rest = np.float32(rest - piece)
    return pieces


def dot(a, b):
    return jnp.dot(a, b, preferred_element_type=F32)


def dot_t(a, b):
    return lax.dot_general(a, b, (((1,), (1,)), ((), ())), preferred_element_type=F32)


def attention_kernel(x_ref, mask_ref, bias_ref, g0_ref, g1_ref, wq_ref, wk_ref, wv_ref, wo_ref, wr_ref, eid_ref,
                     h1_ref, b_ref, gate_ref, q_s, k_s, v_s, c_s):
    seq, dim = x_ref.shape
    heads = bias_ref.shape[0]
    head = dim // heads
    lanes = 2 * head
    hid = x_ref[...].astype(F32)
    inv = lax.rsqrt(jnp.mean(hid * hid, axis=-1, keepdims=True) + NORM_EPS)
    normed = (hid * inv * g0_ref[...]).astype(BF16)
    pairs = heads // 2
    for w_ref, rows_s in ((wq_ref, q_s), (wk_ref, k_s), (wv_ref, v_s)):
        rows = dot(normed, w_ref[...]).astype(BF16)
        for pair in range(pairs):
            rows_s[pair] = rows[:, pair * lanes:(pair + 1) * lanes]
    lane = lax.broadcasted_iota(jnp.int32, (seq, lanes), 1)
    hi, mid, lo = neg_pieces()
    piece = jnp.where(lane == 0, hi, jnp.where(lane == 1, mid, jnp.where(lane == 2, lo, 0.0)))
    key_mask = jnp.where(mask_ref[...] > 0, 0.0, piece).astype(BF16)
    ones = jnp.ones((seq, lanes), BF16)
    zero = jnp.zeros((seq, lanes), BF16)
    low = lane < head

    def one_pair(pair):
        keys = jnp.concatenate([k_s[pair], key_mask], axis=1)
        vals = v_s[pair]
        outs = []
        for half in range(2):
            keep = low if half == 0 else jnp.logical_not(low)
            query = jnp.concatenate([jnp.where(keep, q_s[pair], zero), ones], axis=1)
            scores = dot_t(query, keys) + bias_ref[2 * pair + half]
            top = jnp.max(scores, axis=-1, keepdims=True)
            probs = jnp.exp(scores - top)
            total = jnp.sum(probs, axis=-1, keepdims=True)
            outs.append(dot(probs.astype(BF16), vals) * (1.0 / total))
        c_s[pair] = jnp.where(low, outs[0], outs[1]).astype(BF16)

    group = PAIRS_PER_STEP

    def some_pairs(i, carry):
        for n in range(group):
            one_pair(i * group + n)
        return carry
    lax.fori_loop(0, pairs // group, some_pairs, 0)
    context = jnp.concatenate([c_s[pair] for pair in range(pairs)], axis=1)
    h1 = (hid + dot(context, wo_ref[...])).astype(BF16)
    h1_ref[...] = h1
    hid1 = h1.astype(F32)
    inv1 = lax.rsqrt(jnp.mean(hid1 * hid1, axis=-1, keepdims=True) + NORM_EPS)
    rows = hid1 * inv1 * g1_ref[...]
    rows1 = rows.astype(BF16)
    b_ref[...] = rows1
    rest = rows - rows1.astype(F32)
    rows2 = rest.astype(BF16)
    rows3 = (rest - rows2.astype(F32)).astype(BF16)
    acc = dot(rows1, wr_ref[0]) + (dot(rows2, wr_ref[1]) + dot(rows3, wr_ref[2]))
    nexp = wr_ref.shape[2] // 8
    logits = acc[:, :nexp] + (acc[:, nexp:2 * nexp] + acc[:, 2 * nexp:3 * nexp])
    expo = jnp.exp(logits - jnp.max(logits, axis=-1, keepdims=True))
    ids = lax.broadcasted_iota(jnp.int32, expo.shape, 1)
    picked = jnp.sum(jnp.where(ids == eid_ref[...], expo, 0.0), axis=-1, keepdims=True)
    gate_ref[...] = picked / jnp.sum(expo, axis=-1, keepdims=True)


def attention(hidden, mask_col, rel_bias, g0, g1, wq, wk, wv, wo, wr, eid_col, seq):
    toks, dim = hidden.shape
    heads = rel_bias.shape[0]
    tok_spec = pl.BlockSpec((seq, dim), lambda s: (s, 0))
    col_spec = pl.BlockSpec((seq, 1), lambda s: (s, 0))

    def whole(arr):
        return pl.BlockSpec(arr.shape, lambda s: (0,) * arr.ndim, pipeline_mode=pl.Buffered(1))

    nseq = toks // seq
    return pl.pallas_call(
        attention_kernel,
        grid=(nseq,),
        in_specs=[tok_spec, col_spec, whole(rel_bias), whole(g0), whole(g1), whole(wq), whole(wk), whole(wv), whole(wo),
                  whole(wr), col_spec],
        out_specs=[tok_spec, tok_spec, col_spec],
        out_shape=[jax.ShapeDtypeStruct((toks, dim), BF16), jax.ShapeDtypeStruct((toks, dim), BF16),
                   jax.ShapeDtypeStruct((toks, 1), F32)],
        scratch_shapes=[pltpu.VMEM((heads // 2, seq, 2 * dim // heads), BF16)] * 4,
        compiler_params=pltpu.CompilerParams(dimension_semantics=("arbitrary",), vmem_limit_bytes=60 * 2**20),
        cost_estimate=pl.CostEstimate(flops=toks * dim * dim * 8 + toks * seq * dim * 4, bytes_accessed=toks * dim * 6,
                                      transcendentals=toks * seq * heads),
        name="attention",
    )(hidden, mask_col, rel_bias, g0, g1, wq, wk, wv, wo, wr, eid_col)


def pack_kernel(reg_ref, dst_ref, cnt_ref, b_ref, pos_ref, out_ref, acc_s, srt_s, sem, *, nexp, cap):
    step = pl.program_id(0)
    seq, dim = b_ref.shape
    rows = srt_s.shape[0]
    chunk = 256

    @pl.when(step == 0)
    def _():
        def clear(i, carry):
            acc_s[pl.ds(pl.multiple_of(i * chunk, chunk), chunk), :] = jnp.zeros((chunk, dim), BF16)
            return carry
        lax.fori_loop(0, acc_s.shape[0] // chunk, clear, 0)

    pos = pos_ref[0]
    last = step * nexp + nexp - 1
    used = (reg_ref[last] + cnt_ref[last]) * TILE
    for c in range(rows // chunk):
        @pl.when(used > c * chunk)
        def _():
            ids = lax.broadcasted_iota(jnp.int32, (chunk, seq), 0) + c * chunk
            pick = jnp.where(ids == pos, 1.0, 0.0).astype(BF16)
            srt_s[c * chunk:(c + 1) * chunk, :] = dot(pick, b_ref[...]).astype(BF16)

    for e in range(nexp):
        base = step * nexp + e
        src0, dst0 = reg_ref[base] * TILE, dst_ref[base] * TILE + e * cap

        def move(i, carry):
            src = pl.ds(pl.multiple_of(src0 + i * TILE, TILE), TILE)
            dst = pl.ds(pl.multiple_of(dst0 + i * TILE, TILE), TILE)
            acc_s[dst, :] = acc_s[dst, :] + srt_s[src, :]
            return carry
        lax.fori_loop(0, cnt_ref[base], move, 0)

    @pl.when(step == pl.num_programs(0) - 1)
    def _():
        copy = pltpu.make_async_copy(acc_s, out_ref, sem)
        copy.start()
        copy.wait()


def pack(reg, dst, cnt, b, pos_row, nexp, cap):
    toks, dim = b.shape
    nseq, _, seq = pos_row.shape
    rows = seq + 2 * nexp * TILE
    return pl.pallas_call(
        functools.partial(pack_kernel, nexp=nexp, cap=cap),
        grid_spec=pltpu.PrefetchScalarGridSpec(
            num_scalar_prefetch=3,
            grid=(nseq,),
            in_specs=[pl.BlockSpec((seq, dim), lambda s, *_: (s, 0)), pl.BlockSpec((1, 1, seq), lambda s, *_: (s, 0, 0))],
            out_specs=pl.BlockSpec(memory_space=pl.ANY),
            scratch_shapes=[pltpu.VMEM((nexp * cap, dim), BF16), pltpu.VMEM((rows, dim), BF16), pltpu.SemaphoreType.DMA(())],
        ),
        out_shape=jax.ShapeDtypeStruct((nexp * cap, dim), BF16),
        compiler_params=pltpu.CompilerParams(dimension_semantics=("arbitrary",), vmem_limit_bytes=60 * 2**20),
        cost_estimate=pl.CostEstimate(flops=2 * nseq * rows * seq * dim, bytes_accessed=nexp * cap * dim * 2, transcendentals=0),
        name="pack",
    )(reg, dst, cnt, b, pos_row)


def combine_kernel(reg_ref, dst_ref, cnt_ref, ret_ref, h1_ref, gate_ref, pos_ref, out_ref, srt_s, *, nexp, cap):
    step = pl.program_id(0)
    seq, dim = h1_ref.shape
    rows = srt_s.shape[0]

    @pl.when(step == 0)
    def _():
        srt_s[...] = jnp.zeros_like(srt_s)

    for e in range(nexp):
        base = step * nexp + e
        src0, dst0 = reg_ref[base] * TILE, dst_ref[base] * TILE + e * cap

        def move(i, carry):
            src = pl.ds(pl.multiple_of(src0 + i * TILE, TILE), TILE)
            dst = pl.ds(pl.multiple_of(dst0 + i * TILE, TILE), TILE)
            srt_s[src, :] = ret_ref[dst, :]
            return carry
        lax.fori_loop(0, cnt_ref[base], move, 0)

    ids = lax.broadcasted_iota(jnp.int32, (seq, rows), 1)
    pick = jnp.where(ids == pos_ref[...], 1.0, 0.0).astype(BF16)
    back = dot(pick, srt_s[...])
    out_ref[...] = (h1_ref[...].astype(F32) + gate_ref[...] * back).astype(BF16)


def combine(reg, dst, cnt, returned, h1, gate, pos_col, nexp, cap, seq):
    toks, dim = h1.shape
    rows = seq + 2 * nexp * TILE
    tok_spec = pl.BlockSpec((seq, dim), lambda s, *_: (s, 0))
    col_spec = pl.BlockSpec((seq, 1), lambda s, *_: (s, 0))
    return pl.pallas_call(
        functools.partial(combine_kernel, nexp=nexp, cap=cap),
        grid_spec=pltpu.PrefetchScalarGridSpec(
            num_scalar_prefetch=3,
            grid=(toks // seq,),
            in_specs=[pl.BlockSpec(returned.shape, lambda s, *_: (0, 0), pipeline_mode=pl.Buffered(1)), tok_spec, col_spec, col_spec],
            out_specs=tok_spec,
            scratch_shapes=[pltpu.VMEM((rows, dim), BF16)],
        ),
        out_shape=jax.ShapeDtypeStruct((toks, dim), BF16),
        compiler_params=pltpu.CompilerParams(dimension_semantics=("arbitrary",), vmem_limit_bytes=60 * 2**20),
        cost_estimate=pl.CostEstimate(flops=2 * toks * rows * dim, bytes_accessed=nexp * cap * dim * 2, transcendentals=0),
        name="combine",
    )(reg, dst, cnt, returned, h1, gate, pos_col)


def peer_of(k, count):
    me = lax.axis_index('ep')
    chip, core = me // 2, me % 2
    return ((chip + k // 2) % (count // 2)) * 2 + (core + k % 2) % 2


def source_of(k, count):
    me = lax.axis_index('ep')
    chip, core = me // 2, me % 2
    return ((chip + count // 2 - k // 2) % (count // 2)) * 2 + (core + k % 2) % 2


def expert_rows(x, up, down, acc_s, inner):
    step = min(inner, 768)

    def part(f, carry):
        cols = pl.ds(pl.multiple_of(f * step, step), step)
        act = jnp.maximum(dot(x, up[:, cols]), 0.0).astype(BF16)
        acc_s[...] = acc_s[...] + dot(act, down[cols, :])
        return carry
    acc_s[...] = jnp.zeros_like(acc_s)
    lax.fori_loop(0, inner // step, part, 0)
    return acc_s[...].astype(BF16)


def exchange_kernel(*refs, layer, count, local, away, block, stay):
    if stay:
        (packed_ref, up_ref, down_ref, ups_ref, downs_ref, ret_ref, recv_s, up_s, down_s, acc_s, w_sem, send_sem, recv_sem, back_sem,
         home_sem, x_h, up_h, down_h, in_sem, out_sem) = refs
    else:
        (packed_ref, up_ref, down_ref, ret_ref, recv_s, up_s, down_s, acc_s, w_sem, send_sem, recv_sem, back_sem,
         home_sem) = refs
    cap, dim = packed_ref.shape[1], packed_ref.shape[2]
    inner = up_s.shape[2]
    halves = cap // block
    pieces = away * halves
    me = lax.axis_index('ep')

    def part(p):
        return p // halves, pl.ds(pl.multiple_of((p % halves) * block, block), block)

    def outgoing(k, p):
        peer = peer_of(k, count)
        j, rows = part(p)
        return pltpu.make_async_remote_copy(
            src_ref=packed_ref.at[peer * local + j, rows], dst_ref=recv_s.at[k, j, rows], send_sem=send_sem.at[k, p],
            recv_sem=recv_sem.at[k, p], device_id={'ep': peer}, device_id_type=pl.DeviceIdType.MESH)

    def homing(k, p):
        j, rows = part(p)
        return pltpu.make_async_remote_copy(
            src_ref=recv_s.at[k, j, rows], dst_ref=ret_ref.at[me * local + j, rows], send_sem=back_sem.at[k, p],
            recv_sem=home_sem.at[k, p], device_id={'ep': source_of(k, count)}, device_id_type=pl.DeviceIdType.MESH)

    def own_in(p):
        j, rows = part(p)
        return pltpu.make_async_copy(packed_ref.at[me * local + j, rows], recv_s.at[0, j, rows], recv_sem.at[0, p])

    def own_out(p):
        j, rows = part(p)
        return pltpu.make_async_copy(recv_s.at[0, j, rows], ret_ref.at[me * local + j, rows], back_sem.at[0, p])

    def weights(j):
        return (pltpu.make_async_copy(up_ref.at[layer, j], up_s.at[j], w_sem.at[0, j]),
                pltpu.make_async_copy(down_ref.at[layer, j], down_s.at[j], w_sem.at[1, j]))

    def home_in(n):
        slot = n % 2
        return (pltpu.make_async_copy(packed_ref.at[(n // stay) * local + away + n % stay], x_h.at[slot], in_sem.at[0, slot]),
                pltpu.make_async_copy(ups_ref.at[n], up_h.at[slot], in_sem.at[1, slot]),
                pltpu.make_async_copy(downs_ref.at[n], down_h.at[slot], in_sem.at[2, slot]))

    def home_out(n):
        return pltpu.make_async_copy(x_h.at[n % 2], ret_ref.at[(n // stay) * local + away + n % stay], out_sem.at[n % 2])

    barrier = pltpu.get_barrier_semaphore()
    for k in range(1, count):
        pl.semaphore_signal(barrier, inc=1, device_id={'ep': peer_of(k, count)}, device_id_type=pl.DeviceIdType.MESH)
    pl.semaphore_wait(barrier, count - 1)

    def start_out(i, carry):
        outgoing(1 + i % (count - 1), i // (count - 1)).start()
        return carry
    lax.fori_loop(0, pieces * (count - 1), start_out, 0)
    for p in range(pieces):
        own_in(p).start()
    for j in range(away):
        for copy in weights(j):
            copy.start()
    if stay:
        for copy in home_in(0):
            copy.start()
    for j in range(away):
        for copy in weights(j):
            copy.wait()

    def order(t):
        u = jnp.maximum(t - pieces, 0)
        own = t < pieces
        return jnp.where(own, 0, 1 + u % (count - 1)), jnp.where(own, t, u // (count - 1))

    def send_back(t):
        @pl.when(t < pieces)
        def _():
            own_out(t).start()

        @pl.when(t >= pieces)
        def _():
            u = t - pieces
            homing(1 + u % (count - 1), u // (count - 1)).start()

    def work(t, carry):
        @pl.when(t < pieces)
        def _():
            own_in(t).wait()

        @pl.when(t >= pieces)
        def _():
            u = t - pieces
            outgoing(1 + u % (count - 1), u // (count - 1)).wait_recv()

        k, p = order(t)
        j, rows = part(p)
        recv_s[k, j, rows, :] = expert_rows(recv_s[k, j, rows, :], up_s.at[j], down_s.at[j], acc_s, inner)

        @pl.when(t > 0)
        def _():
            send_back(t - 1)

        if stay:
            n, i = t // halves, t % halves
            slot = n % 2

            @pl.when(i == 0)
            def _():
                for copy in home_in(n):
                    copy.wait()

            @pl.when(jnp.logical_and(i == 1, n > 0))
            def _():
                home_out(n - 1).wait()

            @pl.when(jnp.logical_and(i == 1, n + 1 < count * stay))
            def _():
                for copy in home_in(n + 1):
                    copy.start()

            mine = pl.ds(pl.multiple_of(i * block, block), block)
            x_h[slot, mine, :] = expert_rows(x_h[slot, mine, :], up_h.at[slot], down_h.at[slot], acc_s, inner)

            @pl.when(i == halves - 1)
            def _():
                home_out(n).start()
        return carry
    total = pieces * count
    lax.fori_loop(0, total, work, 0)
    send_back(total - 1)

    def drain(i, carry):
        k, p = 1 + i % (count - 1), i // (count - 1)
        outgoing(k, p).wait_send()
        back = homing(k, p)
        back.wait_send()
        back.wait_recv()
        return carry
    lax.fori_loop(0, pieces * (count - 1), drain, 0)
    for p in range(pieces):
        own_out(p).wait()
    if stay:
        home_out(count * stay - 1).wait()


def exchange_ffn(packed, w_in, w_out, layer, count, away, ups=None, downs=None, block=256):
    nexp, cap, dim = packed.shape
    local, inner = w_in.shape[1], w_in.shape[3]
    pieces = away * (cap // block)
    stay = 0 if ups is None else local - away
    assert stay in (0, away) and cap // block > 2
    dma = pltpu.SemaphoreType.DMA
    scratch = [pltpu.VMEM((count, away, cap, dim), BF16), pltpu.VMEM((away, dim, inner), BF16),
               pltpu.VMEM((away, inner, dim), BF16), pltpu.VMEM((block, dim), F32), dma((2, away)),
               dma((count, pieces)), dma((count, pieces)), dma((count, pieces)), dma((count, pieces))]
    operands = [packed, w_in, w_out]
    if stay:
        scratch += [pltpu.VMEM((2, cap, dim), BF16), pltpu.VMEM((2, dim, inner), BF16), pltpu.VMEM((2, inner, dim), BF16),
                    dma((3, 2)), dma((2,))]
        operands += [ups, downs]
    return pl.pallas_call(
        functools.partial(exchange_kernel, layer=layer, count=count, local=local, away=away, block=block, stay=stay),
        in_specs=[pl.BlockSpec(memory_space=pl.ANY)] * len(operands),
        out_specs=pl.BlockSpec(memory_space=pl.ANY),
        out_shape=jax.ShapeDtypeStruct(packed.shape, BF16),
        scratch_shapes=scratch,
        compiler_params=pltpu.CompilerParams(collective_id=layer, has_side_effects=True, vmem_limit_bytes=60 * 2**20),
        cost_estimate=pl.CostEstimate(flops=4 * count * (away + stay) * cap * dim * inner, bytes_accessed=nexp * cap * dim * 4,
                                      transcendentals=0),
        name="exchange_ffn",
    )(*operands)


def home_kernel(fill_ref, x_ref, up_ref, down_ref, ret_ref, out_ref, acc_s, *, local, away, block):
    here = pl.program_id(0)
    e = (here // (local - away)) * local + away + here % (local - away)
    inner = up_ref.shape[1]

    def work(i, carry):
        rows = pl.ds(pl.multiple_of(i * block, block), block)
        out_ref[rows, :] = expert_rows(x_ref[rows, :], up_ref, down_ref, acc_s, inner)
        return carry
    lax.fori_loop(0, (fill_ref[e] + block - 1) // block, work, 0)


def home_ffn(fill, packed, up, down, ret, local, away, block=256):
    nexp, cap, dim = packed.shape
    here, inner = up.shape[0], up.shape[2]
    stay = local - away
    row_spec = pl.BlockSpec((None, cap, dim), lambda e, *_: ((e // stay) * local + away + e % stay, 0, 0))
    return pl.pallas_call(
        functools.partial(home_kernel, local=local, away=away, block=block),
        grid_spec=pltpu.PrefetchScalarGridSpec(
            num_scalar_prefetch=1,
            grid=(here,),
            in_specs=[row_spec, pl.BlockSpec((None, dim, inner), lambda e, *_: (e, 0, 0)),
                      pl.BlockSpec((None, inner, dim), lambda e, *_: (e, 0, 0)), pl.BlockSpec(memory_space=pl.ANY)],
            out_specs=row_spec,
            scratch_shapes=[pltpu.VMEM((block, dim), F32)],
        ),
        out_shape=jax.ShapeDtypeStruct(packed.shape, BF16),
        input_output_aliases={4: 0},
        compiler_params=pltpu.CompilerParams(dimension_semantics=("arbitrary",), vmem_limit_bytes=60 * 2**20),
        cost_estimate=pl.CostEstimate(flops=2 * here * cap * dim * inner, bytes_accessed=here * cap * dim * 4, transcendentals=0),
        name="home_ffn",
    )(fill, packed, up, down, ret)


def routing(expert_idx, nexp, cap):
    layers, nseq, seq = expert_idx.shape
    hot = expert_idx[..., None] == jnp.arange(nexp, dtype=jnp.int32)
    tri = (jnp.arange(seq)[:, None] > jnp.arange(seq)[None, :]).astype(BF16)
    before = jnp.einsum('ut,lste->lsue', tri, hot.astype(BF16), preferred_element_type=F32).astype(jnp.int32)
    count = jnp.sum(hot.astype(jnp.int32), axis=2)
    prior = jnp.arange(nseq)[:, None] > jnp.arange(nseq)[None, :]
    start = jnp.sum(jnp.where(prior[None, :, :, None], count[:, None], 0), axis=2)
    kept = jnp.clip(cap - start, 0, count)
    off = start % TILE
    tiles = jnp.where(kept > 0, (off + kept + TILE - 1) // TILE, 0)
    lower = jnp.arange(nexp)[:, None] > jnp.arange(nexp)[None, :]
    reg = jnp.sum(jnp.where(lower[None, None], tiles[:, :, None, :], 0), axis=3)
    dst = jnp.minimum(start, cap - 1) // TILE
    place = jnp.where(before < kept[:, :, None, :], (reg * TILE + off)[:, :, None, :] + before, 1 << 20)
    pos = jnp.sum(jnp.where(hot, place, 0), axis=3)
    return reg, dst, tiles, pos, jnp.sum(kept, axis=1)


def split_router(w_router):
    layers, dim, nexp = w_router.shape
    w1 = lax.reduce_precision(w_router, 8, 7)
    w2 = lax.reduce_precision(w_router - w1, 8, 7)
    w3 = lax.reduce_precision(w_router - w1 - w2, 8, 7)
    zero = jnp.zeros_like(w1)
    rows = [[w1, w2, w3], [w1, w2, zero], [w1, zero, zero]]
    out = jnp.stack([jnp.concatenate(r + [zero] * 5, axis=2) for r in rows], axis=1)
    return out.astype(BF16)


def solution(mesh):
    token_spec = P(('dp', 'ep'))

    def per_device(x_in, pad_mask, rel_bias, expert_idx, norm_scale, w_query, w_key, w_value, w_attn_out, w_router, w_in, w_out):
        num_seqs, seq_len, model_dim = x_in.shape
        toks = num_seqs * seq_len
        nexp = w_router.shape[2]
        layers = w_router.shape[0]
        cap = (CAP_FACTOR * toks + nexp - 1) // nexp
        local = w_in.shape[1]
        count = nexp // local
        reg, dst, tiles, pos, fill = routing(expert_idx, nexp, cap)
        wr = split_router(w_router)
        mask_col = pad_mask.reshape(toks, 1)
        hidden = x_in.reshape(toks, model_dim)
        shared = [min(n, local - 1) for n in SHARED]

        def gather(weight, layer, early, after):
            if early is not None:
                weight, _ = lax.optimization_barrier((weight, early))
            own = weight[layer, local - shared[layer]:]
            if after is not None:
                own, _ = lax.optimization_barrier((own, after))
            return lax.all_gather(own, 'ep', axis=0, tiled=True)

        early = after = None
        for layer in range(layers):
            tables = [t[layer].reshape(num_seqs * nexp) for t in (reg, dst, tiles)]
            if shared[layer]:
                ups, downs = (gather(w, layer, early, after) for w in (w_in, w_out))
            h1, b, gate = attention(hidden, mask_col, rel_bias, norm_scale[layer, 0][None], norm_scale[layer, 1][None],
                                    w_query[layer], w_key[layer], w_value[layer], w_attn_out[layer], wr[layer],
                                    expert_idx[layer].reshape(toks, 1), seq_len)
            early = gate[:8]
            packed = pack(*tables, b, pos[layer].reshape(num_seqs, 1, seq_len), nexp, cap)
            packed = packed.reshape(nexp, cap, model_dim)
            away = local - shared[layer]
            if shared[layer] and layer == layers - 1:
                returned = exchange_ffn(packed, w_in, w_out, layer, count, away, ups, downs)
            else:
                returned = exchange_ffn(packed, w_in, w_out, layer, count, away)
                after = returned[0, :TILE, :128]
                if shared[layer]:
                    returned = home_ffn(fill[layer], packed, ups, downs, returned, local, away)
            hidden = combine(*tables, returned.reshape(nexp * cap, model_dim), h1, gate, pos[layer].reshape(toks, 1), nexp, cap, seq_len)
        return hidden.reshape(num_seqs, seq_len, model_dim)

    return jax.shard_map(per_device, mesh=mesh, in_specs=(token_spec, token_spec, P(), P(None, ('dp', 'ep')), P(), P(), P(), P(), P(), P(), P(None, 'ep'), P(None, 'ep')), out_specs=token_spec, check_vma=False)
```

```python
import functools

import jax
import jax.numpy as jnp
import numpy as np
from jax import lax
from jax.experimental import pallas as pl
from jax.experimental.pallas import tpu as pltpu
from jax.sharding import PartitionSpec as P

NORM_EPS = 1e-6
NEG_BIG = -1e9
CAP_FACTOR = 2
TILE = 16
PAIRS_PER_STEP = 3
SHARED = (1, 1)
BF16 = jnp.bfloat16
F32 = jnp.float32


def neg_pieces():
    pieces, rest = [], np.float32(NEG_BIG)
    for _ in range(3):
        piece = np.float32(np.asarray(rest, jnp.bfloat16))
        pieces.append(float(piece))
        rest = np.float32(rest - piece)
    return pieces


def dot(a, b):
    return jnp.dot(a, b, preferred_element_type=F32)


def dot_t(a, b):
    return lax.dot_general(a, b, (((1,), (1,)), ((), ())), preferred_element_type=F32)


def attention_kernel(x_ref, mask_ref, bias_ref, g0_ref, g1_ref, wq_ref, wk_ref, wv_ref, wo_ref, wr_ref, eid_ref,
                     h1_ref, b_ref, gate_ref, q_s, k_s, v_s, c_s):
    seq, dim = x_ref.shape
    heads = bias_ref.shape[0]
    head = dim // heads
    lanes = 2 * head
    hid = x_ref[...].astype(F32)
    inv = lax.rsqrt(jnp.mean(hid * hid, axis=-1, keepdims=True) + NORM_EPS)
    normed = (hid * inv * g0_ref[...]).astype(BF16)
    pairs = heads // 2
    for w_ref, rows_s in ((wq_ref, q_s), (wk_ref, k_s), (wv_ref, v_s)):
        rows = dot(normed, w_ref[...]).astype(BF16)
        for pair in range(pairs):
            rows_s[pair] = rows[:, pair * lanes:(pair + 1) * lanes]
    lane = lax.broadcasted_iota(jnp.int32, (seq, lanes), 1)
    hi, mid, lo = neg_pieces()
    piece = jnp.where(lane == 0, hi, jnp.where(lane == 1, mid, jnp.where(lane == 2, lo, 0.0)))
    key_mask = jnp.where(mask_ref[...] > 0, 0.0, piece).astype(BF16)
    ones = jnp.ones((seq, lanes), BF16)
    zero = jnp.zeros((seq, lanes), BF16)
    low = lane < head

    def one_pair(pair):
        keys = jnp.concatenate([k_s[pair], key_mask], axis=1)
        vals = v_s[pair]
        outs = []
        for half in range(2):
            keep = low if half == 0 else jnp.logical_not(low)
            query = jnp.concatenate([jnp.where(keep, q_s[pair], zero), ones], axis=1)
            scores = dot_t(query, keys) + bias_ref[2 * pair + half]
            top = jnp.max(scores, axis=-1, keepdims=True)
            probs = jnp.exp(scores - top)
            total = jnp.sum(probs, axis=-1, keepdims=True)
            outs.append(dot(probs.astype(BF16), vals) * (1.0 / total))
        c_s[pair] = jnp.where(low, outs[0], outs[1]).astype(BF16)

    group = PAIRS_PER_STEP

    def some_pairs(i, carry):
        for n in range(group):
            one_pair(i * group + n)
        return carry
    lax.fori_loop(0, pairs // group, some_pairs, 0)
    context = jnp.concatenate([c_s[pair] for pair in range(pairs)], axis=1)
    h1 = (hid + dot(context, wo_ref[...])).astype(BF16)
    h1_ref[...] = h1
    hid1 = h1.astype(F32)
    inv1 = lax.rsqrt(jnp.mean(hid1 * hid1, axis=-1, keepdims=True) + NORM_EPS)
    rows = hid1 * inv1 * g1_ref[...]
    rows1 = rows.astype(BF16)
    b_ref[...] = rows1
    rest = rows - rows1.astype(F32)
    rows2 = rest.astype(BF16)
    rows3 = (rest - rows2.astype(F32)).astype(BF16)
    acc = dot(rows1, wr_ref[0]) + (dot(rows2, wr_ref[1]) + dot(rows3, wr_ref[2]))
    nexp = wr_ref.shape[2] // 8
    logits = acc[:, :nexp] + (acc[:, nexp:2 * nexp] + acc[:, 2 * nexp:3 * nexp])
    expo = jnp.exp(logits - jnp.max(logits, axis=-1, keepdims=True))
    ids = lax.broadcasted_iota(jnp.int32, expo.shape, 1)
    picked = jnp.sum(jnp.where(ids == eid_ref[...], expo, 0.0), axis=-1, keepdims=True)
    gate_ref[...] = picked / jnp.sum(expo, axis=-1, keepdims=True)


def attention(hidden, mask_col, rel_bias, g0, g1, wq, wk, wv, wo, wr, eid_col, seq):
    toks, dim = hidden.shape
    heads = rel_bias.shape[0]
    tok_spec = pl.BlockSpec((seq, dim), lambda s: (s, 0))
    col_spec = pl.BlockSpec((seq, 1), lambda s: (s, 0))

    def whole(arr):
        return pl.BlockSpec(arr.shape, lambda s: (0,) * arr.ndim, pipeline_mode=pl.Buffered(1))

    nseq = toks // seq
    return pl.pallas_call(
        attention_kernel,
        grid=(nseq,),
        in_specs=[tok_spec, col_spec, whole(rel_bias), whole(g0), whole(g1), whole(wq), whole(wk), whole(wv), whole(wo),
                  whole(wr), col_spec],
        out_specs=[tok_spec, tok_spec, col_spec],
        out_shape=[jax.ShapeDtypeStruct((toks, dim), BF16), jax.ShapeDtypeStruct((toks, dim), BF16),
                   jax.ShapeDtypeStruct((toks, 1), F32)],
        scratch_shapes=[pltpu.VMEM((heads // 2, seq, 2 * dim // heads), BF16)] * 4,
        compiler_params=pltpu.CompilerParams(dimension_semantics=("arbitrary",), vmem_limit_bytes=60 * 2**20),
        cost_estimate=pl.CostEstimate(flops=toks * dim * dim * 8 + toks * seq * dim * 4, bytes_accessed=toks * dim * 6,
                                      transcendentals=toks * seq * heads),
        name="attention",
    )(hidden, mask_col, rel_bias, g0, g1, wq, wk, wv, wo, wr, eid_col)


def pack_kernel(reg_ref, dst_ref, cnt_ref, b_ref, pos_ref, out_ref, acc_s, srt_s, sem, *, nexp, cap):
    step = pl.program_id(0)
    seq, dim = b_ref.shape
    rows = srt_s.shape[0]
    chunk = 256

    @pl.when(step == 0)
    def _():
        def clear(i, carry):
            acc_s[pl.ds(pl.multiple_of(i * chunk, chunk), chunk), :] = jnp.zeros((chunk, dim), BF16)
            return carry
        lax.fori_loop(0, acc_s.shape[0] // chunk, clear, 0)

    pos = pos_ref[0]
    last = step * nexp + nexp - 1
    used = (reg_ref[last] + cnt_ref[last]) * TILE
    for c in range(rows // chunk):
        @pl.when(used > c * chunk)
        def _():
            ids = lax.broadcasted_iota(jnp.int32, (chunk, seq), 0) + c * chunk
            pick = jnp.where(ids == pos, 1.0, 0.0).astype(BF16)
            srt_s[c * chunk:(c + 1) * chunk, :] = dot(pick, b_ref[...]).astype(BF16)

    for e in range(nexp):
        base = step * nexp + e
        src0, dst0 = reg_ref[base] * TILE, dst_ref[base] * TILE + e * cap

        def move(i, carry):
            src = pl.ds(pl.multiple_of(src0 + i * TILE, TILE), TILE)
            dst = pl.ds(pl.multiple_of(dst0 + i * TILE, TILE), TILE)
            acc_s[dst, :] = acc_s[dst, :] + srt_s[src, :]
            return carry
        lax.fori_loop(0, cnt_ref[base], move, 0)

    @pl.when(step == pl.num_programs(0) - 1)
    def _():
        copy = pltpu.make_async_copy(acc_s, out_ref, sem)
        copy.start()
        copy.wait()


def pack(reg, dst, cnt, b, pos_row, nexp, cap):
    toks, dim = b.shape
    nseq, _, seq = pos_row.shape
    rows = seq + 2 * nexp * TILE
    return pl.pallas_call(
        functools.partial(pack_kernel, nexp=nexp, cap=cap),
        grid_spec=pltpu.PrefetchScalarGridSpec(
            num_scalar_prefetch=3,
            grid=(nseq,),
            in_specs=[pl.BlockSpec((seq, dim), lambda s, *_: (s, 0)), pl.BlockSpec((1, 1, seq), lambda s, *_: (s, 0, 0))],
            out_specs=pl.BlockSpec(memory_space=pl.ANY),
            scratch_shapes=[pltpu.VMEM((nexp * cap, dim), BF16), pltpu.VMEM((rows, dim), BF16), pltpu.SemaphoreType.DMA(())],
        ),
        out_shape=jax.ShapeDtypeStruct((nexp * cap, dim), BF16),
        compiler_params=pltpu.CompilerParams(dimension_semantics=("arbitrary",), vmem_limit_bytes=60 * 2**20),
        cost_estimate=pl.CostEstimate(flops=2 * nseq * rows * seq * dim, bytes_accessed=nexp * cap * dim * 2, transcendentals=0),
        name="pack",
    )(reg, dst, cnt, b, pos_row)


def combine_kernel(reg_ref, dst_ref, cnt_ref, ret_ref, h1_ref, gate_ref, pos_ref, out_ref, srt_s, *, nexp, cap):
    step = pl.program_id(0)
    seq, dim = h1_ref.shape
    rows = srt_s.shape[0]

    @pl.when(step == 0)
    def _():
        srt_s[...] = jnp.zeros_like(srt_s)

    for e in range(nexp):
        base = step * nexp + e
        src0, dst0 = reg_ref[base] * TILE, dst_ref[base] * TILE + e * cap

        def move(i, carry):
            src = pl.ds(pl.multiple_of(src0 + i * TILE, TILE), TILE)
            dst = pl.ds(pl.multiple_of(dst0 + i * TILE, TILE), TILE)
            srt_s[src, :] = ret_ref[dst, :]
            return carry
        lax.fori_loop(0, cnt_ref[base], move, 0)

    ids = lax.broadcasted_iota(jnp.int32, (seq, rows), 1)
    pick = jnp.where(ids == pos_ref[...], 1.0, 0.0).astype(BF16)
    back = dot(pick, srt_s[...])
    out_ref[...] = (h1_ref[...].astype(F32) + gate_ref[...] * back).astype(BF16)


def combine(reg, dst, cnt, returned, h1, gate, pos_col, nexp, cap, seq):
    toks, dim = h1.shape
    rows = seq + 2 * nexp * TILE
    tok_spec = pl.BlockSpec((seq, dim), lambda s, *_: (s, 0))
    col_spec = pl.BlockSpec((seq, 1), lambda s, *_: (s, 0))
    return pl.pallas_call(
        functools.partial(combine_kernel, nexp=nexp, cap=cap),
        grid_spec=pltpu.PrefetchScalarGridSpec(
            num_scalar_prefetch=3,
            grid=(toks // seq,),
            in_specs=[pl.BlockSpec(returned.shape, lambda s, *_: (0, 0), pipeline_mode=pl.Buffered(1)), tok_spec, col_spec, col_spec],
            out_specs=tok_spec,
            scratch_shapes=[pltpu.VMEM((rows, dim), BF16)],
        ),
        out_shape=jax.ShapeDtypeStruct((toks, dim), BF16),
        compiler_params=pltpu.CompilerParams(dimension_semantics=("arbitrary",), vmem_limit_bytes=60 * 2**20),
        cost_estimate=pl.CostEstimate(flops=2 * toks * rows * dim, bytes_accessed=nexp * cap * dim * 2, transcendentals=0),
        name="combine",
    )(reg, dst, cnt, returned, h1, gate, pos_col)


def peer_of(k, count):
    me = lax.axis_index('ep')
    chip, core = me // 2, me % 2
    return ((chip + k // 2) % (count // 2)) * 2 + (core + k % 2) % 2


def source_of(k, count):
    me = lax.axis_index('ep')
    chip, core = me // 2, me % 2
    return ((chip + count // 2 - k // 2) % (count // 2)) * 2 + (core + k % 2) % 2


def expert_rows(x, up, down, acc_s, inner):
    step = min(inner, 768)

    def part(f, carry):
        cols = pl.ds(pl.multiple_of(f * step, step), step)
        act = jnp.maximum(dot(x, up[:, cols]), 0.0).astype(BF16)
        acc_s[...] = acc_s[...] + dot(act, down[cols, :])
        return carry
    acc_s[...] = jnp.zeros_like(acc_s)
    lax.fori_loop(0, inner // step, part, 0)
    return acc_s[...].astype(BF16)


def exchange_kernel(*refs, layer, count, local, away, block, stay):
    if stay:
        (packed_ref, up_ref, down_ref, ups_ref, downs_ref, ret_ref, recv_s, up_s, down_s, acc_s, w_sem, send_sem, recv_sem, back_sem,
         home_sem, x_h, up_h, down_h, in_sem, out_sem) = refs
    else:
        (packed_ref, up_ref, down_ref, ret_ref, next_up_ref, next_down_ref, recv_s, up_s, down_s, acc_s, w_sem, send_sem, recv_sem,
         back_sem, home_sem, next_up_s, next_down_s, next_sem) = refs
    cap, dim = packed_ref.shape[1], packed_ref.shape[2]
    inner = up_s.shape[2]
    halves = cap // block
    pieces = away * halves
    me = lax.axis_index('ep')

    def part(p):
        return p // halves, pl.ds(pl.multiple_of((p % halves) * block, block), block)

    def outgoing(k, p):
        peer = peer_of(k, count)
        j, rows = part(p)
        return pltpu.make_async_remote_copy(
            src_ref=packed_ref.at[peer * local + j, rows], dst_ref=recv_s.at[k, j, rows], send_sem=send_sem.at[k, p],
            recv_sem=recv_sem.at[k, p], device_id={'ep': peer}, device_id_type=pl.DeviceIdType.MESH)

    def homing(k, p):
        j, rows = part(p)
        return pltpu.make_async_remote_copy(
            src_ref=recv_s.at[k, j, rows], dst_ref=ret_ref.at[me * local + j, rows], send_sem=back_sem.at[k, p],
            recv_sem=home_sem.at[k, p], device_id={'ep': source_of(k, count)}, device_id_type=pl.DeviceIdType.MESH)

    def own_in(p):
        j, rows = part(p)
        return pltpu.make_async_copy(packed_ref.at[me * local + j, rows], recv_s.at[0, j, rows], recv_sem.at[0, p])

    def own_out(p):
        j, rows = part(p)
        return pltpu.make_async_copy(recv_s.at[0, j, rows], ret_ref.at[me * local + j, rows], back_sem.at[0, p])

    def weights(j):
        return (pltpu.make_async_copy(up_ref.at[layer, j], up_s.at[j], w_sem.at[0, j]),
                pltpu.make_async_copy(down_ref.at[layer, j], down_s.at[j], w_sem.at[1, j]))

    def home_in(n):
        slot = n % 2
        return (pltpu.make_async_copy(packed_ref.at[(n // stay) * local + away + n % stay], x_h.at[slot], in_sem.at[0, slot]),
                pltpu.make_async_copy(ups_ref.at[n], up_h.at[slot], in_sem.at[1, slot]),
                pltpu.make_async_copy(downs_ref.at[n], down_h.at[slot], in_sem.at[2, slot]))

    def home_out(n):
        return pltpu.make_async_copy(x_h.at[n % 2], ret_ref.at[(n // stay) * local + away + n % stay], out_sem.at[n % 2])

    def share_in():
        mine = pl.ds(away, local - away)
        return (pltpu.make_async_copy(up_ref.at[layer + 1, mine], next_up_s, next_sem.at[0]),
                pltpu.make_async_copy(down_ref.at[layer + 1, mine], next_down_s, next_sem.at[1]))

    def share_out():
        return (pltpu.make_async_copy(next_up_s, next_up_ref, next_sem.at[2]),
                pltpu.make_async_copy(next_down_s, next_down_ref, next_sem.at[3]))

    barrier = pltpu.get_barrier_semaphore()
    for k in range(1, count):
        pl.semaphore_signal(barrier, inc=1, device_id={'ep': peer_of(k, count)}, device_id_type=pl.DeviceIdType.MESH)
    pl.semaphore_wait(barrier, count - 1)

    def start_out(i, carry):
        outgoing(1 + i % (count - 1), i // (count - 1)).start()
        return carry
    lax.fori_loop(0, pieces * (count - 1), start_out, 0)
    for p in range(pieces):
        own_in(p).start()
    for j in range(away):
        for copy in weights(j):
            copy.start()
    for copy in (home_in(0) if stay else share_in()):
        copy.start()
    for j in range(away):
        for copy in weights(j):
            copy.wait()
    if not stay:
        for copy in share_in():
            copy.wait()
        for copy in share_out():
            copy.start()

    def order(t):
        u = jnp.maximum(t - pieces, 0)
        own = t < pieces
        return jnp.where(own, 0, 1 + u % (count - 1)), jnp.where(own, t, u // (count - 1))

    def send_back(t):
        @pl.when(t < pieces)
        def _():
            own_out(t).start()

        @pl.when(t >= pieces)
        def _():
            u = t - pieces
            homing(1 + u % (count - 1), u // (count - 1)).start()

    def work(t, carry):
        @pl.when(t < pieces)
        def _():
            own_in(t).wait()

        @pl.when(t >= pieces)
        def _():
            u = t - pieces
            outgoing(1 + u % (count - 1), u // (count - 1)).wait_recv()

        k, p = order(t)
        j, rows = part(p)
        recv_s[k, j, rows, :] = expert_rows(recv_s[k, j, rows, :], up_s.at[j], down_s.at[j], acc_s, inner)

        @pl.when(t > 0)
        def _():
            send_back(t - 1)

        if stay:
            n, i = t // halves, t % halves
            slot = n % 2

            @pl.when(i == 0)
            def _():
                for copy in home_in(n):
                    copy.wait()

            @pl.when(jnp.logical_and(i == 1, n > 0))
            def _():
                home_out(n - 1).wait()

            @pl.when(jnp.logical_and(i == 1, n + 1 < count * stay))
            def _():
                for copy in home_in(n + 1):
                    copy.start()

            mine = pl.ds(pl.multiple_of(i * block, block), block)
            x_h[slot, mine, :] = expert_rows(x_h[slot, mine, :], up_h.at[slot], down_h.at[slot], acc_s, inner)

            @pl.when(i == halves - 1)
            def _():
                home_out(n).start()
        return carry
    total = pieces * count
    lax.fori_loop(0, total, work, 0)
    send_back(total - 1)

    def drain(i, carry):
        k, p = 1 + i % (count - 1), i // (count - 1)
        outgoing(k, p).wait_send()
        back = homing(k, p)
        back.wait_send()
        back.wait_recv()
        return carry
    lax.fori_loop(0, pieces * (count - 1), drain, 0)
    for p in range(pieces):
        own_out(p).wait()
    if stay:
        home_out(count * stay - 1).wait()
    else:
        for copy in share_out():
            copy.wait()


def exchange_ffn(packed, w_in, w_out, layer, count, away, ups=None, downs=None, block=256):
    nexp, cap, dim = packed.shape
    local, inner = w_in.shape[1], w_in.shape[3]
    pieces = away * (cap // block)
    stay = 0 if ups is None else local - away
    assert stay in (0, away) and cap // block > 2
    dma = pltpu.SemaphoreType.DMA
    scratch = [pltpu.VMEM((count, away, cap, dim), BF16), pltpu.VMEM((away, dim, inner), BF16),
               pltpu.VMEM((away, inner, dim), BF16), pltpu.VMEM((block, dim), F32), dma((2, away)),
               dma((count, pieces)), dma((count, pieces)), dma((count, pieces)), dma((count, pieces))]
    operands = [packed, w_in, w_out]
    results = [jax.ShapeDtypeStruct(packed.shape, BF16)]
    if not stay:
        kept = local - away
        results += [jax.ShapeDtypeStruct((kept, dim, inner), BF16), jax.ShapeDtypeStruct((kept, inner, dim), BF16)]
        scratch += [pltpu.VMEM((kept, dim, inner), BF16), pltpu.VMEM((kept, inner, dim), BF16), dma((4,))]
    else:
        scratch += [pltpu.VMEM((2, cap, dim), BF16), pltpu.VMEM((2, dim, inner), BF16), pltpu.VMEM((2, inner, dim), BF16),
                    dma((3, 2)), dma((2,))]
        operands += [ups, downs]
    return pl.pallas_call(
        functools.partial(exchange_kernel, layer=layer, count=count, local=local, away=away, block=block, stay=stay),
        in_specs=[pl.BlockSpec(memory_space=pl.ANY)] * len(operands),
        out_specs=[pl.BlockSpec(memory_space=pl.ANY)] * len(results),
        out_shape=results,
        scratch_shapes=scratch,
        compiler_params=pltpu.CompilerParams(collective_id=layer, has_side_effects=True, vmem_limit_bytes=60 * 2**20),
        cost_estimate=pl.CostEstimate(flops=4 * count * (away + stay) * cap * dim * inner, bytes_accessed=nexp * cap * dim * 4,
                                      transcendentals=0),
        name="exchange_ffn",
    )(*operands)


def home_kernel(fill_ref, x_ref, up_ref, down_ref, ret_ref, out_ref, acc_s, *, local, away, block):
    here = pl.program_id(0)
    e = (here // (local - away)) * local + away + here % (local - away)
    inner = up_ref.shape[1]

    def work(i, carry):
        rows = pl.ds(pl.multiple_of(i * block, block), block)
        out_ref[rows, :] = expert_rows(x_ref[rows, :], up_ref, down_ref, acc_s, inner)
        return carry
    lax.fori_loop(0, (fill_ref[e] + block - 1) // block, work, 0)


def home_ffn(fill, packed, up, down, ret, local, away, block=256):
    nexp, cap, dim = packed.shape
    here, inner = up.shape[0], up.shape[2]
    stay = local - away
    row_spec = pl.BlockSpec((None, cap, dim), lambda e, *_: ((e // stay) * local + away + e % stay, 0, 0))
    return pl.pallas_call(
        functools.partial(home_kernel, local=local, away=away, block=block),
        grid_spec=pltpu.PrefetchScalarGridSpec(
            num_scalar_prefetch=1,
            grid=(here,),
            in_specs=[row_spec, pl.BlockSpec((None, dim, inner), lambda e, *_: (e, 0, 0)),
                      pl.BlockSpec((None, inner, dim), lambda e, *_: (e, 0, 0)), pl.BlockSpec(memory_space=pl.ANY)],
            out_specs=row_spec,
            scratch_shapes=[pltpu.VMEM((block, dim), F32)],
        ),
        out_shape=jax.ShapeDtypeStruct(packed.shape, BF16),
        input_output_aliases={4: 0},
        compiler_params=pltpu.CompilerParams(dimension_semantics=("arbitrary",), vmem_limit_bytes=60 * 2**20),
        cost_estimate=pl.CostEstimate(flops=2 * here * cap * dim * inner, bytes_accessed=here * cap * dim * 4, transcendentals=0),
        name="home_ffn",
    )(fill, packed, up, down, ret)


def routing(expert_idx, nexp, cap):
    layers, nseq, seq = expert_idx.shape
    hot = expert_idx[..., None] == jnp.arange(nexp, dtype=jnp.int32)
    tri = (jnp.arange(seq)[:, None] > jnp.arange(seq)[None, :]).astype(BF16)
    before = jnp.einsum('ut,lste->lsue', tri, hot.astype(BF16), preferred_element_type=F32).astype(jnp.int32)
    count = jnp.sum(hot.astype(jnp.int32), axis=2)
    prior = jnp.arange(nseq)[:, None] > jnp.arange(nseq)[None, :]
    start = jnp.sum(jnp.where(prior[None, :, :, None], count[:, None], 0), axis=2)
    kept = jnp.clip(cap - start, 0, count)
    off = start % TILE
    tiles = jnp.where(kept > 0, (off + kept + TILE - 1) // TILE, 0)
    lower = jnp.arange(nexp)[:, None] > jnp.arange(nexp)[None, :]
    reg = jnp.sum(jnp.where(lower[None, None], tiles[:, :, None, :], 0), axis=3)
    dst = jnp.minimum(start, cap - 1) // TILE
    place = jnp.where(before < kept[:, :, None, :], (reg * TILE + off)[:, :, None, :] + before, 1 << 20)
    pos = jnp.sum(jnp.where(hot, place, 0), axis=3)
    return reg, dst, tiles, pos, jnp.sum(kept, axis=1)


def split_router(w_router):
    layers, dim, nexp = w_router.shape
    w1 = lax.reduce_precision(w_router, 8, 7)
    w2 = lax.reduce_precision(w_router - w1, 8, 7)
    w3 = lax.reduce_precision(w_router - w1 - w2, 8, 7)
    zero = jnp.zeros_like(w1)
    rows = [[w1, w2, w3], [w1, w2, zero], [w1, zero, zero]]
    out = jnp.stack([jnp.concatenate(r + [zero] * 5, axis=2) for r in rows], axis=1)
    return out.astype(BF16)


def solution(mesh):
    token_spec = P(('dp', 'ep'))

    def per_device(x_in, pad_mask, rel_bias, expert_idx, norm_scale, w_query, w_key, w_value, w_attn_out, w_router, w_in, w_out):
        num_seqs, seq_len, model_dim = x_in.shape
        toks = num_seqs * seq_len
        nexp = w_router.shape[2]
        layers = w_router.shape[0]
        cap = (CAP_FACTOR * toks + nexp - 1) // nexp
        local = w_in.shape[1]
        count = nexp // local
        reg, dst, tiles, pos, fill = routing(expert_idx, nexp, cap)
        wr = split_router(w_router)
        mask_col = pad_mask.reshape(toks, 1)
        hidden = x_in.reshape(toks, model_dim)
        shared = [min(n, local - 1) for n in SHARED]

        own = [w[0, local - shared[0]:] for w in (w_in, w_out)]
        for layer in range(layers):
            tables = [t[layer].reshape(num_seqs * nexp) for t in (reg, dst, tiles)]
            ups, downs = (lax.all_gather(w, 'ep', axis=0, tiled=True) for w in own)
            h1, b, gate = attention(hidden, mask_col, rel_bias, norm_scale[layer, 0][None], norm_scale[layer, 1][None],
                                    w_query[layer], w_key[layer], w_value[layer], w_attn_out[layer], wr[layer],
                                    expert_idx[layer].reshape(toks, 1), seq_len)
            packed = pack(*tables, b, pos[layer].reshape(num_seqs, 1, seq_len), nexp, cap)
            packed = packed.reshape(nexp, cap, model_dim)
            away = local - shared[layer]
            if layer == layers - 1:
                returned, = exchange_ffn(packed, w_in, w_out, layer, count, away, ups, downs)
            else:
                returned, *own = exchange_ffn(packed, w_in, w_out, layer, count, away)
                returned = home_ffn(fill[layer], packed, ups, downs, returned, local, away)
            hidden = combine(*tables, returned.reshape(nexp * cap, model_dim), h1, gate, pos[layer].reshape(toks, 1), nexp, cap, seq_len)
        return hidden.reshape(num_seqs, seq_len, model_dim)

    return jax.shard_map(per_device, mesh=mesh, in_specs=(token_spec, token_spec, P(), P(None, ('dp', 'ep')), P(), P(), P(), P(), P(), P(), P(None, 'ep'), P(None, 'ep')), out_specs=token_spec, check_vma=False)
```
